32 devices in a mesh: grp: 4 (over y, x), col: 8 (over z, core).
Axes of the slice: x: 2, y: 2, z: 4, core: 2. Of those that a mesh axis runs over, the one named last changes fastest.
Arguments:
- panels: bfloat16 [32, 4, 512, 512], P('col', None, 'grp'), may hold values from -1.296875 to 1.296875
- parent: float32 [32, 512, 512], P('col', 'grp'), may hold values from -6 to 6
- src_block: int32 [8, 40], P('col'), may hold values from 0 to 39, each once within a row
- dest_owner: int32 [320, 1], P('col'), may hold values from 0 to 7; in each aligned block of 40 rows (0 to 39, 40 to 79, ...) at most 7 rows name the same one
- target: int32 [320], P('col'), may hold values from 0 to 3
- counts: int32 [8], P('col'), may hold values from 20 to 40, as said below
Outputs:
- assembled: float32 [32, 512, 512], P('col', 'grp')
The draws below stay inside these ranges and needn't reach their ends.
Inputs may be any that keep to these rules, and one draw needn't show every extreme that they name: `src_block`: each row of a column rank is a permutation of the 40 block pairs. `dest_owner`: among the 40 slots of one column rank at most 7 name the same owner. The live slots of a rank are its first counts[c]; some rank has all 40 live.
All inputs are finite; a program needn't handle non-finite values.
Results may differ from the reference program's by a relative error of at most 0.0026.
Values may be sent and summed in bfloat16 or wider, within the bound.
A program may use at most 128 MiB of HBM per device.

```python
import math
import jax
import jax.numpy as jnp
import numpy as np
from jax import lax

WIDTH = 512
BLOCK = 512
ROW_BLOCKS = 4
FRONTS = 4
TARGETS = 4
PAIRS = 10
SLOTS = 40
CAPACITY = 7
N_COL = 8


def draw_counts(key, part):
    values = jax.random.randint(key, (N_COL,), SLOTS // 2, SLOTS + 1).astype(jnp.int32)
    chosen = jax.random.randint(jax.random.fold_in(key, 7), (), 0, N_COL)
    return values.at[chosen].set(SLOTS)


def set_ends(drawn, own_key, least, high):
    index_at = [jax.random.randint(jax.random.fold_in(own_key, axis), (), 0, length) for axis, length in enumerate(drawn.shape)]
    widest = drawn.shape.index(max(drawn.shape))
    next_to = index_at[:widest] + [(index_at[widest] + 1) % drawn.shape[widest]] + index_at[widest + 1:]
    return drawn.at[tuple(index_at)].set(least).at[tuple(next_to)].set(high)


def level_of(stream_key, shape, cuts, low, top_value):
    def one(position, shards_of):
        steps = jax.random.uniform(jax.random.fold_in(jax.random.fold_in(stream_key, 6), position), (shards_of,), jnp.float32, low / len(cuts), top_value / len(cuts))
        return jnp.repeat(jnp.exp(steps), shape[position] // shards_of).reshape((-1,) + (1,) * (len(shape) - position - 1))

    factor_of = one(*cuts[0])
    for cut in cuts[1:]:
        factor_of = factor_of * one(*cut)
    return factor_of


def shared_out(stream_key, own, number, rows, amount, top, bound, slope):
    ranking = jax.random.permutation(stream_key, amount)
    crowded, common = load_shares(amount, rows * top, bound, slope, True), load_shares(amount, rows * top, bound, slope, False)
    places = jnp.arange(amount)

    def named(lengths, turn):
        used = int((lengths > 0).sum())
        fixed = max(1, used // 4)
        passed = fixed + (places - fixed + turn * (used - fixed)) % max(1, amount - fixed)
        return jnp.zeros((amount,), jnp.int32).at[ranking[jnp.where(places < fixed, places, passed)]].set(jnp.asarray(lengths, jnp.int32))

    lengths = jnp.where(number % 4 == 0, named(crowded, number // 4), named(common, number - number // 4 - 1))
    mixed = jax.random.permutation(jax.random.fold_in(own, 3), amount)
    giver, sink = mixed[0:amount // 2 * 2:2], mixed[1:amount // 2 * 2:2]
    slack = jnp.minimum(lengths[giver] - 1, bound - lengths[sink]) // 2
    slack = jnp.where((giver == ranking[0]) | (sink == ranking[0]) | (lengths[sink] == 0), 0, jnp.maximum(slack, 0))
    passed = jax.random.randint(jax.random.fold_in(own, 4), (amount // 2,), 0, 1 << 20) % (slack + 1)
    lengths = lengths.at[giver].add(-passed).at[sink].add(passed)
    members = jnp.searchsorted(jnp.cumsum(lengths), jnp.arange(rows * top), side="right").astype(jnp.int32)
    listing = members.reshape(top, rows).T
    listing = listing[jax.random.permutation(jax.random.fold_in(own, 1), rows)]
    turn = jax.random.randint(jax.random.fold_in(own, 2), (rows, 1), 0, top)
    return jnp.take_along_axis(listing, (jnp.arange(top)[None, :] + turn) % top, axis=1)


def load_shares(amount, total, most, skew, full):
    portions = [(1 << 20) // math.isqrt(rank ** skew) + 1 for rank in range(1, amount + 1)]
    largest = most if full else min(most, max(-(-total // amount), total * portions[0] // sum(portions)))
    least = 1 if total - largest >= amount - 1 else 0
    given, rest = [largest] + [least] * (amount - 1), total - largest - least * (amount - 1)
    while rest > 0:
        candidates = [i for i in range(1, amount) if given[i] < largest] or [i for i in range(1, amount) if given[i] < most]
        whole, remaining = sum([portions[i] for i in candidates]), rest
        for i in candidates:
            addition = min(most - given[i], max(1, remaining * portions[i] // whole), rest)
            given[i] = given[i] + addition
            rest = rest - addition
    return np.array(given)


def centred(stream_key, shape, spread, most, shards=(), kind=jnp.bfloat16):
    result = jax.random.normal(stream_key, shape, jnp.float32) * spread
    if len(shards) > 0:
        result = level_of(stream_key, shape, shards, -0.22, 0.18) * result
    return jnp.clip(result, min=-most, max=most).astype(kind)


def setup_inputs(seed: int = 0) -> dict:
    streams_of = jax.random.split(jax.random.key(seed), 7)
    panels = centred(streams_of[0], (N_COL * FRONTS, ROW_BLOCKS, BLOCK, WIDTH), 0.21, 1.296875, ((0, 8), (2, 4)))
    parent = centred(streams_of[1], (N_COL * TARGETS, BLOCK, BLOCK), 1.0, 6.0, ((0, 8), (1, 4)), jnp.float32)
    src_block = jax.vmap(lambda own: jax.random.permutation(own, SLOTS))(jax.random.split(streams_of[2], N_COL)).reshape((N_COL, SLOTS)).astype(jnp.int32)
    dest_owner_keys = jax.random.split(jax.random.fold_in(streams_of[3], 1), (N_COL * SLOTS) // SLOTS)
    dest_owner_turns = jax.random.permutation(jax.random.fold_in(streams_of[3], 3), (N_COL * SLOTS) // SLOTS)
    dest_owner = jax.vmap(lambda own, number: shared_out(jax.random.fold_in(streams_of[3], 2), own, number, SLOTS, N_COL, 1, CAPACITY, 2))(dest_owner_keys, dest_owner_turns).reshape((N_COL * SLOTS, 1))
    target = set_ends(jax.random.randint(streams_of[4], (N_COL * SLOTS,), 0, TARGETS), jax.random.fold_in(streams_of[4], 1), 0, TARGETS - 1).astype(jnp.int32)
    counts = draw_counts(jax.random.fold_in(streams_of[6], 71), 0)
    return dict(panels=panels, parent=parent, src_block=src_block, dest_owner=dest_owner, target=target, counts=counts)


def reference(panels, parent, src_block, dest_owner, target, counts):
    running = parent.astype(jnp.float32)
    slot_index = jnp.arange(SLOTS, dtype=jnp.int32)
    upper_table = jnp.asarray(np.array([a for a in range(ROW_BLOCKS) for b in range(a + 1)], np.int32))
    lower_table = jnp.asarray(np.array([b for a in range(ROW_BLOCKS) for b in range(a + 1)], np.int32))

    def add_device(column_rank, running):
        own_panels = lax.dynamic_slice_in_dim(panels, (column_rank * FRONTS).astype(jnp.int32), FRONTS, 0)
        flat_rows = own_panels.astype(jnp.float32).reshape(FRONTS * ROW_BLOCKS, BLOCK, WIDTH)
        combos = lax.dynamic_index_in_dim(src_block, column_rank, 0, keepdims=False)
        front_of = combos // PAIRS
        within = combos % PAIRS
        left_index = (front_of * ROW_BLOCKS + upper_table[within]).astype(jnp.int32)
        right_index = (front_of * ROW_BLOCKS + lower_table[within]).astype(jnp.int32)
        left_rows = flat_rows[left_index]
        right_rows = flat_rows[right_index]
        updates = jnp.einsum("srw,scw->src", left_rows, right_rows, precision=lax.Precision.HIGHEST)
        updates = updates.astype(jnp.bfloat16).astype(jnp.float32)
        limit = lax.dynamic_index_in_dim(counts, column_rank, 0, keepdims=False)
        is_live = slot_index < limit
        updates = jnp.where(is_live[:, None, None], updates, jnp.zeros_like(updates))
        start = (column_rank * SLOTS).astype(jnp.int32)
        owner_rank = lax.dynamic_slice_in_dim(dest_owner[:, 0], start, SLOTS, 0)
        block_target = lax.dynamic_slice_in_dim(target, start, SLOTS, 0)
        dest_rows = (owner_rank * TARGETS + block_target).astype(jnp.int32)
        return running.at[dest_rows].add(-updates)

    return lax.fori_loop(0, N_COL, add_device, running)
```

```python
import functools

import jax
import jax.numpy as jnp
import numpy as np
from jax import lax
from jax.experimental import pallas as pl
from jax.experimental.pallas import tpu as pltpu
from jax.sharding import PartitionSpec as P

MESH = pl.DeviceIdType.MESH


def place_slots(src_block, dest_owner, target, counts, peer_count, capacity):
    slot_count = src_block.shape[1]
    slot_index = jnp.arange(slot_count, dtype=jnp.int32)
    owner_rank = dest_owner[:, 0]
    matches = (owner_rank[:, None] == jnp.arange(peer_count, dtype=jnp.int32)[None, :]).astype(
        jnp.int32
    )
    earlier = jnp.cumsum(matches, axis=0) - matches
    rank_in = jnp.sum(earlier * matches, axis=1)
    position = owner_rank * capacity + rank_in
    is_live = slot_index < counts[0]
    routed = jnp.zeros((peer_count * capacity,), jnp.int32).at[position].set(target)
    return (src_block[0], position, is_live, routed.reshape(peer_count, capacity))


def pack_updates(flat_updates, chosen, position, is_live, peer_count, capacity):
    picked = flat_updates[chosen]
    picked = jnp.where(is_live[:, None, None], picked, jnp.zeros_like(picked))
    buffer = (
        jnp.zeros((peer_count * capacity,) + picked.shape[1:], picked.dtype)
        .at[position]
        .set(picked)
    )
    return buffer.reshape((peer_count, capacity) + picked.shape[1:])


def assemble(received, labels, targets):
    arrived = received.reshape((-1,) + received.shape[2:])
    flat_labels = labels.reshape(-1)
    select = (flat_labels[None, :] == jnp.arange(targets, dtype=jnp.int32)[:, None]).astype(
        jnp.bfloat16
    )
    return jnp.einsum("tn,nrc->trc", select, arrived, preferred_element_type=jnp.float32)


def pair_products(own_rows, piece_rows):
    blocks = own_rows.shape[1]
    upper_table = np.array([a for a in range(blocks) for b in range(a + 1)], np.int32)
    lower_table = np.array([b for a in range(blocks) for b in range(a + 1)], np.int32)
    left_rows = own_rows[:, upper_table]
    right_rows = piece_rows[:, lower_table]
    return jnp.einsum(
        "fprw,fpcw->fprc", left_rows, right_rows, preferred_element_type=jnp.float32
    ).astype(jnp.bfloat16)


def slot_table(src_block, dest_owner, target, counts, peer_count, capacity):
    slot_count = src_block.shape[1]
    slot_index = jnp.arange(slot_count, dtype=jnp.int32)
    owner = dest_owner[:, 0]
    earlier = (slot_index[None, :] < slot_index[:, None]) & (owner[None, :] == owner[:, None])
    rank_in = jnp.sum(earlier.astype(jnp.int32), axis=1)
    position = owner * capacity + rank_in
    hit = jnp.arange(peer_count * capacity, dtype=jnp.int32)[:, None] == position[None, :]
    label = jnp.where(slot_index < counts[0], target + 1, 0)
    pair = jnp.stack([src_block[0], label])
    return jnp.sum(jnp.where(hit[None], pair[:, None, :], 0), axis=2)


def kernel(
    chips, capacity, table, own, parent, out,
    from_x, from_y, from_d, product, kept, to_pair, from_pair, to_chip, from_chip,
    x_send, x_recv, y_send, y_recv, dx_send, dx_recv, dy_send, dy_recv,
    p_send, p_recv, z_send, z_recv,
):
    fronts, blocks, quarter, _ = own.shape
    targets = parent.shape[0]
    pairs = blocks * (blocks + 1) // 2
    g, c = lax.axis_index("grp"), lax.axis_index("col")
    gy, gx = g // 2, g % 2
    z, core = c // 2, c % 2
    x_peer = gy * 2 + (1 - gx)
    y_peer = (1 - gy) * 2 + gx
    d_peer = 3 - g
    to_x, to_y = {"grp": x_peer, "col": c}, {"grp": y_peer, "col": c}
    to_core = {"grp": g, "col": z * 2 + 1 - core}
    far = [lax.rem(z + hop, chips) for hop in range(1, chips)]
    to_far = [{"grp": g, "col": chip * 2 + core} for chip in far]

    barrier = pltpu.get_barrier_semaphore()
    peers = [to_x, to_y, to_core] + to_far
    for peer in peers:
        pl.semaphore_signal(barrier, inc=1, device_id=peer, device_id_type=MESH)
    pl.semaphore_wait(barrier, len(peers))

    def remote(src, dst, send, recv, device):
        return pltpu.make_async_remote_copy(
            src_ref=src, dst_ref=dst, send_sem=send, recv_sem=recv,
            device_id=device, device_id_type=MESH,
        )

    half = fronts // 2
    first, second = list(range(half)), list(range(half, fronts))
    x_copy = [
        remote(own.at[f], from_x.at[f], x_send.at[f], x_recv.at[f], to_x) for f in range(fronts)
    ]
    y_copy = [
        remote(own.at[f], from_y.at[f], y_send.at[f], y_recv.at[f], to_y) for f in range(fronts)
    ]
    for f, h in zip(first + second, second + first):
        x_copy[f].start()
        y_copy[h].start()
    dy_copy = [
        remote(from_x.at[f], from_d.at[f], dy_send.at[f], dy_recv.at[f], to_y) for f in first
    ]
    dx_copy = [
        remote(from_y.at[f], from_d.at[f], dx_send.at[f - half], dx_recv.at[f - half], to_x)
        for f in second
    ]

    def products(rows):
        def front(f, carry):
            for b in range(blocks):
                left = own[f, b:].reshape((blocks - b) * quarter, own.shape[3])
                made = lax.dot_general(
                    left, rows[f, b], (((1,), (1,)), ((), ())),
                    preferred_element_type=jnp.float32,
                ).astype(jnp.bfloat16)
                for a in range(b, blocks):
                    at = f * pairs + a * (a + 1) // 2 + b
                    product[at] = made[(a - b) * quarter:(a - b + 1) * quarter]
            return carry

        lax.fori_loop(0, fronts, front, 0)

    tile = 32

    def select(parity, store):
        def chip(zz, carry):
            base = (zz * 2 + parity) * capacity
            chosen = [table[0, base + k] for k in range(capacity)]
            label = [table[1, base + k] for k in range(capacity)]
            weight = [
                [jnp.where(label[k] == t + 1, 1.0, 0.0).astype(jnp.float32) for t in range(targets)]
                for k in range(capacity)
            ]

            def rows(i, carry):
                at = pl.ds(pl.multiple_of(i * tile, tile), tile)
                taken = [product[chosen[k], at, :].astype(jnp.float32) for k in range(capacity)]
                for t in range(targets):
                    total = taken[0] * weight[0][t]
                    for k in range(1, capacity):
                        total = total + taken[k] * weight[k][t]
                    store(zz, t, at, total)
                return carry

            return lax.fori_loop(0, quarter // tile, rows, carry)

        lax.fori_loop(0, chips, chip, 0)

    def columns(member):
        return pl.ds(pl.multiple_of(member * quarter, quarter), quarter)

    p_copy = [
        remote(to_pair.at[n], from_pair.at[n], p_send.at[n], p_recv.at[n], to_core)
        for n in range(4)
    ]
    z_copy = [
        [
            remote(to_chip.at[n, h], from_chip.at[n, h], z_send.at[n, h], z_recv.at[n, h], to_far[h])
            for h in range(chips - 1)
        ]
        for n in range(4)
    ]

    def chunk(n, rows, member):
        products(rows)

        def store_pair(zz, t, at, total):
            to_pair[n, zz, t, at, :] = total.astype(jnp.bfloat16)

        def store_kept(zz, t, at, total):
            kept[zz, t, at, :] = total

        select(1 - core, store_pair)
        p_copy[n].start()
        select(core, store_kept)
        p_copy[n].wait_recv()
        for h in range(chips - 1):
            to_chip[n, h] = (kept[far[h]] + from_pair[n, far[h]].astype(jnp.float32)).astype(
                jnp.bfloat16
            )
            z_copy[n][h].start()
        at = columns(member)
        out[:, :, at] = parent[:, :, at] - (kept[z] + from_pair[n, z].astype(jnp.float32))

    def finish(n, member):
        at = columns(member)
        total = out[:, :, at]
        for h in range(chips - 1):
            z_copy[n][h].wait_recv()
        for h in range(chips - 1):
            total = total - from_chip[n, h].astype(jnp.float32)
        out[:, :, at] = total

    chunk(0, own, g)
    for i in range(half):
        x_copy[first[i]].wait_recv()
        dy_copy[i].start()
        y_copy[second[i]].wait_recv()
        dx_copy[i].start()
    finish(0, g)
    for f in second:
        x_copy[f].wait_recv()
    chunk(1, from_x, x_peer)
    for f in first:
        y_copy[f].wait_recv()
    chunk(2, from_y, y_peer)
    for copy in dy_copy + dx_copy:
        copy.wait_recv()
    chunk(3, from_d, d_peer)
    finish(1, x_peer)
    finish(2, y_peer)
    finish(3, d_peer)
    for copy in x_copy + y_copy + dy_copy + dx_copy + p_copy:
        copy.wait_send()
    for row in z_copy:
        for copy in row:
            copy.wait_send()


def fused(panels, parent, table, chips, capacity):
    fronts, blocks, quarter, width = panels.shape
    targets = parent.shape[0]
    pairs = blocks * (blocks + 1) // 2
    half = fronts // 2
    rows = pltpu.VMEM(panels.shape, panels.dtype)
    dma = pltpu.SemaphoreType.DMA
    return pl.pallas_call(
        functools.partial(kernel, chips, capacity),
        out_shape=jax.ShapeDtypeStruct(parent.shape, parent.dtype),
        in_specs=[
            pl.BlockSpec(memory_space=pltpu.SMEM),
            pl.BlockSpec(memory_space=pltpu.VMEM),
            pl.BlockSpec(memory_space=pltpu.VMEM),
        ],
        out_specs=pl.BlockSpec(memory_space=pltpu.VMEM),
        scratch_shapes=[
            rows, rows, rows,
            pltpu.VMEM((fronts * pairs, quarter, quarter), jnp.bfloat16),
            pltpu.VMEM((chips, targets, quarter, quarter), jnp.float32),
            pltpu.VMEM((4, chips, targets, quarter, quarter), jnp.bfloat16),
            pltpu.VMEM((4, chips, targets, quarter, quarter), jnp.bfloat16),
            pltpu.VMEM((4, chips - 1, targets, quarter, quarter), jnp.bfloat16),
            pltpu.VMEM((4, chips - 1, targets, quarter, quarter), jnp.bfloat16),
            dma((fronts,)), dma((fronts,)), dma((fronts,)), dma((fronts,)),
            dma((half,)), dma((half,)), dma((half,)), dma((half,)),
            dma((4,)), dma((4,)), dma((4, chips - 1)), dma((4, chips - 1)),
        ],
        compiler_params=pltpu.CompilerParams(
            collective_id=0, has_side_effects=True, vmem_limit_bytes=60 * 1024 * 1024
        ),
    )(table, panels, parent)


def per_device(panels, parent, src_block, dest_owner, target, counts):
    fronts, blocks, quarter, _ = panels.shape
    pair_count = blocks * (blocks + 1) // 2
    peer_count = lax.axis_size("col")
    slot_count = src_block.shape[1]
    capacity = (slot_count + peer_count - 1) // peer_count + slot_count // (2 * peer_count)
    targets = parent.shape[0]
    if lax.axis_size("grp") == 4 and peer_count % 2 == 0 and targets < capacity:
        table = slot_table(src_block, dest_owner, target, counts, peer_count, capacity)
        return fused(panels, parent, table, peer_count // 2, capacity)
    chosen, position, is_live, routed = place_slots(
        src_block, dest_owner, target, counts, peer_count, capacity
    )
    products = pair_products(panels, lax.all_gather(panels, "grp", axis=2, tiled=True))
    flat_updates = products.reshape(fronts * pair_count, quarter, products.shape[3])
    buffer = pack_updates(flat_updates, chosen, position, is_live, peer_count, capacity)
    received, labels = (
        lax.all_to_all(buffer, "col", split_axis=0, concat_axis=0, tiled=True),
        lax.all_to_all(routed, "col", split_axis=0, concat_axis=0, tiled=True),
    )
    return parent - assemble(received, labels, targets)


def solution(mesh):
    placed = (
        P("col", None, "grp", None),
        P("col", "grp", None),
        P("col", None),
        P("col", None),
        P("col"),
        P("col"),
    )
    return jax.shard_map(
        per_device, mesh=mesh, in_specs=placed, out_specs=P("col", "grp", None), check_vma=False
    )
```

```python
import functools

import jax
import jax.numpy as jnp
import numpy as np
from jax import lax
from jax.experimental import pallas as pl
from jax.experimental.pallas import tpu as pltpu
from jax.sharding import PartitionSpec as P

MESH = pl.DeviceIdType.MESH


def place_slots(src_block, dest_owner, target, counts, peer_count, capacity):
    slot_count = src_block.shape[1]
    slot_index = jnp.arange(slot_count, dtype=jnp.int32)
    owner_rank = dest_owner[:, 0]
    matches = (owner_rank[:, None] == jnp.arange(peer_count, dtype=jnp.int32)[None, :]).astype(
        jnp.int32
    )
    earlier = jnp.cumsum(matches, axis=0) - matches
    rank_in = jnp.sum(earlier * matches, axis=1)
    position = owner_rank * capacity + rank_in
    is_live = slot_index < counts[0]
    routed = jnp.zeros((peer_count * capacity,), jnp.int32).at[position].set(target)
    return (src_block[0], position, is_live, routed.reshape(peer_count, capacity))


def pack_updates(flat_updates, chosen, position, is_live, peer_count, capacity):
    picked = flat_updates[chosen]
    picked = jnp.where(is_live[:, None, None], picked, jnp.zeros_like(picked))
    buffer = (
        jnp.zeros((peer_count * capacity,) + picked.shape[1:], picked.dtype)
        .at[position]
        .set(picked)
    )
    return buffer.reshape((peer_count, capacity) + picked.shape[1:])


def assemble(received, labels, targets):
    arrived = received.reshape((-1,) + received.shape[2:])
    flat_labels = labels.reshape(-1)
    select = (flat_labels[None, :] == jnp.arange(targets, dtype=jnp.int32)[:, None]).astype(
        jnp.bfloat16
    )
    return jnp.einsum("tn,nrc->trc", select, arrived, preferred_element_type=jnp.float32)


def pair_products(own_rows, piece_rows):
    blocks = own_rows.shape[1]
    upper_table = np.array([a for a in range(blocks) for b in range(a + 1)], np.int32)
    lower_table = np.array([b for a in range(blocks) for b in range(a + 1)], np.int32)
    left_rows = own_rows[:, upper_table]
    right_rows = piece_rows[:, lower_table]
    return jnp.einsum(
        "fprw,fpcw->fprc", left_rows, right_rows, preferred_element_type=jnp.float32
    ).astype(jnp.bfloat16)


def kernel(
    chips, capacity, split, src_block, owner, target, counts, own, parent, out,
    table, from_x, from_y, product, kept, summed, to_pair, from_pair, to_chip, from_chip,
    to_back, from_back,
    x_send, x_recv, y_send, y_recv, p_send, p_recv, z_send, z_recv, b_send, b_recv,
):
    fronts, blocks, quarter, width = own.shape
    targets = parent.shape[0]
    pairs = blocks * (blocks + 1) // 2
    slots = src_block.shape[1]
    g, c = lax.axis_index("grp"), lax.axis_index("col")
    gy, gx = g // 2, g % 2
    z, core = c // 2, c % 2
    x_peer = gy * 2 + (1 - gx)
    y_peer = (1 - gy) * 2 + gx
    d_peer = 3 - g
    to_x, to_y = {"grp": x_peer, "col": c}, {"grp": y_peer, "col": c}
    to_core = {"grp": g, "col": z * 2 + 1 - core}
    far = [lax.rem(z + hop, chips) for hop in range(1, chips)]
    to_far = [{"grp": g, "col": chip * 2 + core} for chip in far]

    barrier = pltpu.get_barrier_semaphore()
    peers = [to_x, to_y, to_core] + to_far
    for peer in peers:
        pl.semaphore_signal(barrier, inc=1, device_id=peer, device_id_type=MESH)
    pl.semaphore_wait(barrier, len(peers))

    def remote(src, dst, send, recv, device):
        return pltpu.make_async_remote_copy(
            src_ref=src, dst_ref=dst, send_sem=send, recv_sem=recv,
            device_id=device, device_id_type=MESH,
        )

    piece = quarter // split
    x_copy, y_copy = [], []
    for k in range(split):
        at = pl.ds(k * piece, piece)
        x_copy.append(
            remote(own.at[:, :, at], from_x[k], x_send.at[k], x_recv.at[k], to_x)
        )
        y_copy.append(
            remote(own.at[:, :, at], from_y[k], y_send.at[k], y_recv.at[k], to_y)
        )
        x_copy[k].start()
        y_copy[k].start()

    def list_owner(o, carry):
        def look(s, state):
            count, chosen, label = state
            mine = owner[0, s] == o
            named = jnp.where(s < counts[0], target[0, s] + 1, 0)
            hits = [jnp.logical_and(mine, count == k) for k in range(capacity)]
            return (
                count + jnp.where(mine, 1, 0),
                tuple(jnp.where(hits[k], src_block[0, s], chosen[k]) for k in range(capacity)),
                tuple(jnp.where(hits[k], named, label[k]) for k in range(capacity)),
            )

        none = tuple(jnp.int32(0) for _ in range(capacity))
        _, chosen, label = lax.fori_loop(0, slots, look, (jnp.int32(0), none, none))
        for k in range(capacity):
            table[0, o * capacity + k] = chosen[k]
            table[1, o * capacity + k] = label[k]
        return carry

    lax.fori_loop(0, 2 * chips, list_owner, 0)

    def place(n, source, against, pieces):
        high = quarter // pieces
        share = len(source) // pieces
        return [
            (source[i * share:(i + 1) * share], high, against, n * quarter + i * high)
            for i in range(pieces)
        ]

    units = (
        place(0, [own], [own], 1)
        + place(1, from_x, [own], split)
        + place(2, from_y, [own], split)
        + place(3, from_y, from_x, 2)
    )
    u_own, u_x, u_y = 0, list(range(1, 1 + split)), list(range(1 + split, 1 + 2 * split))
    u_d = [1 + 2 * split, 2 + 2 * split]
    tile = 32

    p_copy, z_copy = [], []
    for u in range(len(units)):
        p_copy.append(remote(to_pair[u], from_pair[u], p_send.at[u], p_recv.at[u], to_core))
        z_copy.append([
            remote(
                to_chip[u].at[h], from_chip[u].at[h],
                z_send.at[u, h], z_recv.at[u, h], to_far[h],
            )
            for h in range(chips - 1)
        ])

    def select(high, parity, store):
        def chip(zz, carry):
            base = (zz * 2 + parity) * capacity
            chosen = [table[0, base + k] for k in range(capacity)]
            label = [table[1, base + k] for k in range(capacity)]
            weight = [
                [jnp.where(label[k] == t + 1, 1.0, 0.0).astype(jnp.float32) for t in range(targets)]
                for k in range(capacity)
            ]

            def rows(i, carry):
                start = pl.multiple_of(i * tile, tile)
                taken = [
                    product[chosen[k], pl.ds(start, tile), :].astype(jnp.float32)
                    for k in range(capacity)
                ]
                for t in range(targets):
                    total = taken[0] * weight[0][t]
                    for k in range(1, capacity):
                        total = total + taken[k] * weight[k][t]
                    store(zz, t, start, total)
                return carry

            return lax.fori_loop(0, high // tile, rows, carry)

        lax.fori_loop(0, chips, chip, 0)

    def make(u, slot):
        source, high, against, _ = units[u]

        def front(f, carry):
            for b in range(blocks):
                left = jnp.concatenate([ref[f, b] for ref in source], axis=0)
                right = jnp.concatenate(
                    [ref[f, a] for a in range(b, blocks) for ref in against], axis=0
                )
                made = lax.dot_general(
                    left, right, (((1,), (1,)), ((), ())),
                    preferred_element_type=jnp.float32,
                ).astype(jnp.bfloat16)
                for a in range(b, blocks):
                    at = f * pairs + a * (a + 1) // 2 + b
                    product[at, :high] = made[:, (a - b) * quarter:(a - b + 1) * quarter]
            return carry

        lax.fori_loop(0, fronts, front, 0)

        def store_pair(zz, t, start, total):
            to_pair[u][zz, t, pl.ds(start, tile), :] = total.astype(jnp.bfloat16)

        def store_kept(zz, t, start, total):
            kept[slot, zz, t, pl.ds(start, tile), :] = total

        select(high, 1 - core, store_pair)
        p_copy[u].start()
        select(high, core, store_kept)

    def pass_on(u, slot):
        _, high, _, row = units[u]
        at = slice(row, row + high)
        p_copy[u].wait_recv()
        for h in range(chips - 1):
            to_chip[u][h] = (
                kept[slot, far[h], :, :high] + from_pair[u][far[h]].astype(jnp.float32)
            ).astype(jnp.bfloat16)
            z_copy[u][h].start()
        summed[:, at] = kept[slot, z, :, :high] + from_pair[u][z].astype(jnp.float32)

    def finish(u):
        _, high, _, row = units[u]
        at = slice(row, row + high)
        for h in range(chips - 1):
            z_copy[u][h].wait_recv()
        total = summed[:, at]
        for h in range(chips - 1):
            total = total + from_chip[u][h].astype(jnp.float32)
        return total

    def settle(u):
        _, high, _, row = units[u]
        summed[:, row:row + high] = finish(u)

    def write(member, total_of):
        at = pl.ds(pl.multiple_of(member * quarter, quarter), quarter)
        for t in range(targets):
            out[t, :, at] = parent[t, :, at] - total_of(t).T

    make(u_own, 0)
    pass_on(u_own, 0)
    for k in range(split - 1):
        x_copy[k].wait_recv()
        make(u_x[k], 0)
        y_copy[k].wait_recv()
        make(u_y[k], 1)
        pass_on(u_x[k], 0)
        pass_on(u_y[k], 1)
    settle(u_own)
    write(g, lambda t: summed[t, :quarter])
    x_copy[-1].wait_recv()
    y_copy[-1].wait_recv()
    make(u_d[0], 0)
    make(u_d[1], 1)
    pass_on(u_d[0], 0)
    make(u_x[-1], 0)
    pass_on(u_d[1], 1)
    make(u_y[-1], 1)
    pass_on(u_x[-1], 0)
    pass_on(u_y[-1], 1)
    for k in range(split - 1):
        settle(u_x[k])
        settle(u_y[k])
    for u in u_d:
        row, high = units[u][3], units[u][1]
        to_back[:, row - 3 * quarter:row - 3 * quarter + high] = finish(u)
    back = remote(to_back, from_back, b_send, b_recv, to_x)
    back.start()
    settle(u_x[-1])
    write(x_peer, lambda t: summed[t, quarter:2 * quarter])
    settle(u_y[-1])
    write(y_peer, lambda t: summed[t, 2 * quarter:3 * quarter])
    back.wait_recv()
    write(d_peer, lambda t: from_back[t])
    for copy in x_copy + y_copy + p_copy + [back]:
        copy.wait_send()
    for row in z_copy:
        for copy in row:
            copy.wait_send()


def fused(panels, parent, src_block, dest_owner, target, counts, chips, capacity):
    fronts, blocks, quarter, width = panels.shape
    targets = parent.shape[0]
    pairs = blocks * (blocks + 1) // 2
    split = 4
    units = 3 + 2 * split
    piece = pltpu.VMEM((fronts, blocks, quarter // split, width), panels.dtype)
    heights = [quarter] + [quarter // split] * (2 * split) + [quarter // 2] * 2

    def buffers(count):
        return [pltpu.VMEM((count, targets, high, quarter), jnp.bfloat16) for high in heights]

    last = (targets, quarter, quarter)
    dma = pltpu.SemaphoreType.DMA
    scalars = pl.BlockSpec(memory_space=pltpu.SMEM)
    arrays = pl.BlockSpec(memory_space=pltpu.VMEM)
    return pl.pallas_call(
        functools.partial(kernel, chips, capacity, split),
        out_shape=jax.ShapeDtypeStruct(parent.shape, parent.dtype),
        in_specs=[scalars] * 4 + [arrays] * 2,
        out_specs=arrays,
        scratch_shapes=[
            pltpu.SMEM((2, 2 * chips * capacity), jnp.int32),
            [piece] * split, [piece] * split,
            pltpu.VMEM((fronts * pairs, quarter, quarter), jnp.bfloat16),
            pltpu.VMEM((2, chips) + last, jnp.float32),
            pltpu.VMEM((targets, 4 * quarter, quarter), jnp.float32),
            buffers(chips), buffers(chips), buffers(chips - 1), buffers(chips - 1),
            pltpu.VMEM(last, jnp.float32),
            pltpu.VMEM(last, jnp.float32),
            dma((split,)), dma((split,)), dma((split,)), dma((split,)),
            dma((units,)), dma((units,)), dma((units, chips - 1)), dma((units, chips - 1)),
            dma, dma,
        ],
        compiler_params=pltpu.CompilerParams(
            collective_id=0, has_side_effects=True, vmem_limit_bytes=60 * 1024 * 1024
        ),
    )(src_block, dest_owner.reshape(1, -1), target.reshape(1, -1), counts, panels, parent)


def per_device(panels, parent, src_block, dest_owner, target, counts):
    fronts, blocks, quarter, _ = panels.shape
    pair_count = blocks * (blocks + 1) // 2
    peer_count = lax.axis_size("col")
    slot_count = src_block.shape[1]
    capacity = (slot_count + peer_count - 1) // peer_count + slot_count // (2 * peer_count)
    targets = parent.shape[0]
    if lax.axis_size("grp") == 4 and peer_count % 2 == 0 and targets < capacity:
        return fused(
            panels, parent, src_block, dest_owner, target, counts, peer_count // 2, capacity
        )
    chosen, position, is_live, routed = place_slots(
        src_block, dest_owner, target, counts, peer_count, capacity
    )
    products = pair_products(panels, lax.all_gather(panels, "grp", axis=2, tiled=True))
    flat_updates = products.reshape(fronts * pair_count, quarter, products.shape[3])
    buffer = pack_updates(flat_updates, chosen, position, is_live, peer_count, capacity)
    received, labels = (
        lax.all_to_all(buffer, "col", split_axis=0, concat_axis=0, tiled=True),
        lax.all_to_all(routed, "col", split_axis=0, concat_axis=0, tiled=True),
    )
    return parent - assemble(received, labels, targets)


def solution(mesh):
    placed = (
        P("col", None, "grp", None),
        P("col", "grp", None),
        P("col", None),
        P("col", None),
        P("col"),
        P("col"),
    )
    return jax.shard_map(
        per_device, mesh=mesh, in_specs=placed, out_specs=P("col", "grp", None), check_vma=False
    )
```

```python
import functools

import jax
import jax.numpy as jnp
import numpy as np
from jax import lax
from jax.experimental import pallas as pl
from jax.experimental.pallas import tpu as pltpu
from jax.sharding import PartitionSpec as P

MESH = pl.DeviceIdType.MESH


def place_slots(src_block, dest_owner, target, counts, peer_count, capacity):
    slot_count = src_block.shape[1]
    slot_index = jnp.arange(slot_count, dtype=jnp.int32)
    owner_rank = dest_owner[:, 0]
    matches = (owner_rank[:, None] == jnp.arange(peer_count, dtype=jnp.int32)[None, :]).astype(
        jnp.int32
    )
    earlier = jnp.cumsum(matches, axis=0) - matches
    rank_in = jnp.sum(earlier * matches, axis=1)
    position = owner_rank * capacity + rank_in
    is_live = slot_index < counts[0]
    routed = jnp.zeros((peer_count * capacity,), jnp.int32).at[position].set(target)
    return (src_block[0], position, is_live, routed.reshape(peer_count, capacity))


def pack_updates(flat_updates, chosen, position, is_live, peer_count, capacity):
    picked = flat_updates[chosen]
    picked = jnp.where(is_live[:, None, None], picked, jnp.zeros_like(picked))
    buffer = (
        jnp.zeros((peer_count * capacity,) + picked.shape[1:], picked.dtype)
        .at[position]
        .set(picked)
    )
    return buffer.reshape((peer_count, capacity) + picked.shape[1:])


def assemble(received, labels, targets):
    arrived = received.reshape((-1,) + received.shape[2:])
    flat_labels = labels.reshape(-1)
    select = (flat_labels[None, :] == jnp.arange(targets, dtype=jnp.int32)[:, None]).astype(
        jnp.bfloat16
    )
    return jnp.einsum("tn,nrc->trc", select, arrived, preferred_element_type=jnp.float32)


def pair_products(own_rows, piece_rows):
    blocks = own_rows.shape[1]
    upper_table = np.array([a for a in range(blocks) for b in range(a + 1)], np.int32)
    lower_table = np.array([b for a in range(blocks) for b in range(a + 1)], np.int32)
    left_rows = own_rows[:, upper_table]
    right_rows = piece_rows[:, lower_table]
    return jnp.einsum(
        "fprw,fpcw->fprc", left_rows, right_rows, preferred_element_type=jnp.float32
    ).astype(jnp.bfloat16)


def kernel(
    chips, capacity, split, src_block, owner, target, counts, own, parent, out,
    table, from_x, from_y, product, kept, summed, to_pair, from_pair, to_chip, from_chip,
    to_back, from_back,
    x_send, x_recv, y_send, y_recv, p_send, p_recv, z_send, z_recv, b_send, b_recv,
):
    fronts, blocks, quarter, width = own.shape
    targets = parent.shape[0]
    pairs = blocks * (blocks + 1) // 2
    slots = src_block.shape[1]
    g, c = lax.axis_index("grp"), lax.axis_index("col")
    gy, gx = g // 2, g % 2
    z, core = c // 2, c % 2
    x_peer = gy * 2 + (1 - gx)
    y_peer = (1 - gy) * 2 + gx
    d_peer = 3 - g
    to_x, to_y = {"grp": x_peer, "col": c}, {"grp": y_peer, "col": c}
    to_core = {"grp": g, "col": z * 2 + 1 - core}
    far = [lax.rem(z + hop, chips) for hop in range(1, chips)]
    to_far = [{"grp": g, "col": chip * 2 + core} for chip in far]

    barrier = pltpu.get_barrier_semaphore()
    peers = [to_x, to_y, to_core] + to_far
    for peer in peers:
        pl.semaphore_signal(barrier, inc=1, device_id=peer, device_id_type=MESH)
    pl.semaphore_wait(barrier, len(peers))

    def remote(src, dst, send, recv, device):
        return pltpu.make_async_remote_copy(
            src_ref=src, dst_ref=dst, send_sem=send, recv_sem=recv,
            device_id=device, device_id_type=MESH,
        )

    piece = quarter // split
    x_copy, y_copy = [], []
    for k in range(split):
        at = pl.ds(k * piece, piece)
        x_copy.append(
            remote(own.at[:, :, at], from_x[k], x_send.at[k], x_recv.at[k], to_x)
        )
        y_copy.append(
            remote(own.at[:, :, at], from_y[k], y_send.at[k], y_recv.at[k], to_y)
        )
        x_copy[k].start()
        y_copy[k].start()

    def list_owner(o, carry):
        def look(s, state):
            count, chosen, label = state
            mine = owner[0, s] == o
            named = jnp.where(s < counts[0], target[0, s] + 1, 0)
            hits = [jnp.logical_and(mine, count == k) for k in range(capacity)]
            return (
                count + jnp.where(mine, 1, 0),
                tuple(jnp.where(hits[k], src_block[0, s], chosen[k]) for k in range(capacity)),
                tuple(jnp.where(hits[k], named, label[k]) for k in range(capacity)),
            )

        none = tuple(jnp.int32(0) for _ in range(capacity))
        _, chosen, label = lax.fori_loop(0, slots, look, (jnp.int32(0), none, none))
        for k in range(capacity):
            table[0, o * capacity + k] = chosen[k]
            table[1, o * capacity + k] = label[k]
        return carry

    lax.fori_loop(0, 2 * chips, list_owner, 0)

    def place(n, source, against, pieces):
        high = quarter // pieces
        share = len(source) // pieces
        return [
            (source[i * share:(i + 1) * share], high, against, n * quarter + i * high)
            for i in range(pieces)
        ]

    units = (
        place(0, [own], [own], 1)
        + [
            ([from_x[k], from_y[k]], 2 * piece, [own], quarter + k * 2 * piece)
            for k in range(split)
        ]
        + place(3, from_y, from_x, 2)
    )
    u_own, u_near, u_d = 0, list(range(1, 1 + split)), [1 + split, 2 + split]
    tile = 32

    p_copy, z_copy = [], []
    for u in range(len(units)):
        p_copy.append(remote(to_pair[u], from_pair[u], p_send.at[u], p_recv.at[u], to_core))
        z_copy.append([
            remote(
                to_chip[u].at[h], from_chip[u].at[h],
                z_send.at[u, h], z_recv.at[u, h], to_far[h],
            )
            for h in range(chips - 1)
        ])

    def select(high, parity, store):
        def chip(zz, carry):
            base = (zz * 2 + parity) * capacity
            chosen = [table[0, base + k] for k in range(capacity)]
            label = [table[1, base + k] for k in range(capacity)]
            weight = [
                [jnp.where(label[k] == t + 1, 1.0, 0.0).astype(jnp.float32) for t in range(targets)]
                for k in range(capacity)
            ]

            def rows(i, carry):
                start = pl.multiple_of(i * tile, tile)
                taken = [
                    product[chosen[k], pl.ds(start, tile), :].astype(jnp.float32)
                    for k in range(capacity)
                ]
                for t in range(targets):
                    total = taken[0] * weight[0][t]
                    for k in range(1, capacity):
                        total = total + taken[k] * weight[k][t]
                    store(zz, t, start, total)
                return carry

            return lax.fori_loop(0, high // tile, rows, carry)

        lax.fori_loop(0, chips, chip, 0)

    def make(u):
        source, high, against, _ = units[u]

        def front(f, carry):
            for b in range(blocks):
                left = jnp.concatenate([ref[f, b] for ref in source], axis=0)
                right = jnp.concatenate(
                    [ref[f, a] for a in range(b, blocks) for ref in against], axis=0
                )
                made = lax.dot_general(
                    left, right, (((1,), (1,)), ((), ())),
                    preferred_element_type=jnp.float32,
                ).astype(jnp.bfloat16)
                for a in range(b, blocks):
                    at = f * pairs + a * (a + 1) // 2 + b
                    product[at, :high] = made[:, (a - b) * quarter:(a - b + 1) * quarter]
            return carry

        lax.fori_loop(0, fronts, front, 0)

        def store_pair(zz, t, start, total):
            to_pair[u][zz, t, pl.ds(start, tile), :] = total.astype(jnp.bfloat16)

        def store_kept(zz, t, start, total):
            kept[zz, t, pl.ds(start, tile), :] = total

        select(high, 1 - core, store_pair)
        p_copy[u].start()
        select(high, core, store_kept)

    def pass_on(u):
        _, high, _, row = units[u]
        at = slice(row, row + high)
        p_copy[u].wait_recv()
        for h in range(chips - 1):
            to_chip[u][h] = (
                kept[far[h], :, :high] + from_pair[u][far[h]].astype(jnp.float32)
            ).astype(jnp.bfloat16)
            z_copy[u][h].start()
        summed[:, at] = kept[z, :, :high] + from_pair[u][z].astype(jnp.float32)

    def finish(u):
        _, high, _, row = units[u]
        at = slice(row, row + high)
        for h in range(chips - 1):
            z_copy[u][h].wait_recv()
        total = summed[:, at]
        for h in range(chips - 1):
            total = total + from_chip[u][h].astype(jnp.float32)
        return total

    def settle(u):
        _, high, _, row = units[u]
        summed[:, row:row + high] = finish(u)

    def write(member, total_of):
        at = pl.ds(pl.multiple_of(member * quarter, quarter), quarter)
        for t in range(targets):
            out[t, :, at] = parent[t, :, at] - total_of(t).T

    def near(first):
        parts = [slice(units[u][3] + first, units[u][3] + first + piece) for u in u_near]
        return lambda t: jnp.concatenate([summed[t, part] for part in parts], axis=0)

    make(u_own)
    pass_on(u_own)
    for k in range(split - 1):
        x_copy[k].wait_recv()
        y_copy[k].wait_recv()
        make(u_near[k])
        pass_on(u_near[k])
    settle(u_own)
    write(g, lambda t: summed[t, :quarter])
    x_copy[-1].wait_recv()
    y_copy[-1].wait_recv()
    for u in u_d + u_near[-1:]:
        make(u)
        pass_on(u)
    for k in range(split - 1):
        settle(u_near[k])
    back = []
    for i, u in enumerate(u_d):
        to_back[i][...] = finish(u)
        back.append(remote(to_back[i], from_back[i], b_send.at[i], b_recv.at[i], to_x))
        back[i].start()
    settle(u_near[-1])
    write(x_peer, near(0))
    write(y_peer, near(piece))
    for copy in back:
        copy.wait_recv()
    write(d_peer, lambda t: jnp.concatenate([ref[t] for ref in from_back], axis=0))
    for copy in x_copy + y_copy + p_copy + back:
        copy.wait_send()
    for row in z_copy:
        for copy in row:
            copy.wait_send()


def fused(panels, parent, src_block, dest_owner, target, counts, chips, capacity):
    fronts, blocks, quarter, width = panels.shape
    targets = parent.shape[0]
    pairs = blocks * (blocks + 1) // 2
    split = 4
    units = 3 + split
    piece = pltpu.VMEM((fronts, blocks, quarter // split, width), panels.dtype)
    heights = [quarter] + [2 * quarter // split] * split + [quarter // 2] * 2

    def buffers(count):
        return [pltpu.VMEM((count, targets, high, quarter), jnp.bfloat16) for high in heights]

    last = (targets, quarter, quarter)
    half = pltpu.VMEM((targets, quarter // 2, quarter), jnp.float32)
    dma = pltpu.SemaphoreType.DMA
    scalars = pl.BlockSpec(memory_space=pltpu.SMEM)
    arrays = pl.BlockSpec(memory_space=pltpu.VMEM)
    return pl.pallas_call(
        functools.partial(kernel, chips, capacity, split),
        out_shape=jax.ShapeDtypeStruct(parent.shape, parent.dtype),
        in_specs=[scalars] * 4 + [arrays] * 2,
        out_specs=arrays,
        scratch_shapes=[
            pltpu.SMEM((2, 2 * chips * capacity), jnp.int32),
            [piece] * split, [piece] * split,
            pltpu.VMEM((fronts * pairs, quarter, quarter), jnp.bfloat16),
            pltpu.VMEM((chips,) + last, jnp.float32),
            pltpu.VMEM((targets, 4 * quarter, quarter), jnp.float32),
            buffers(chips), buffers(chips), buffers(chips - 1), buffers(chips - 1),
            [half, half], [half, half],
            dma((split,)), dma((split,)), dma((split,)), dma((split,)),
            dma((units,)), dma((units,)), dma((units, chips - 1)), dma((units, chips - 1)),
            dma((2,)), dma((2,)),
        ],
        compiler_params=pltpu.CompilerParams(
            collective_id=0, has_side_effects=True, vmem_limit_bytes=60 * 1024 * 1024
        ),
    )(src_block, dest_owner.reshape(1, -1), target.reshape(1, -1), counts, panels, parent)


def per_device(panels, parent, src_block, dest_owner, target, counts):
    fronts, blocks, quarter, _ = panels.shape
    pair_count = blocks * (blocks + 1) // 2
    peer_count = lax.axis_size("col")
    slot_count = src_block.shape[1]
    capacity = (slot_count + peer_count - 1) // peer_count + slot_count // (2 * peer_count)
    targets = parent.shape[0]
    if lax.axis_size("grp") == 4 and peer_count % 2 == 0 and targets < capacity:
        return fused(
            panels, parent, src_block, dest_owner, target, counts, peer_count // 2, capacity
        )
    chosen, position, is_live, routed = place_slots(
        src_block, dest_owner, target, counts, peer_count, capacity
    )
    products = pair_products(panels, lax.all_gather(panels, "grp", axis=2, tiled=True))
    flat_updates = products.reshape(fronts * pair_count, quarter, products.shape[3])
    buffer = pack_updates(flat_updates, chosen, position, is_live, peer_count, capacity)
    received, labels = (
        lax.all_to_all(buffer, "col", split_axis=0, concat_axis=0, tiled=True),
        lax.all_to_all(routed, "col", split_axis=0, concat_axis=0, tiled=True),
    )
    return parent - assemble(received, labels, targets)


def solution(mesh):
    placed = (
        P("col", None, "grp", None),
        P("col", "grp", None),
        P("col", None),
        P("col", None),
        P("col"),
        P("col"),
    )
    return jax.shard_map(
        per_device, mesh=mesh, in_specs=placed, out_specs=P("col", "grp", None), check_vma=False
    )
```
